32 devices in a mesh: dp: 8 (over y, x, core), mp: 4 (over z).
Axes of the slice: x: 2, y: 2, z: 4, core: 2. Of those that a mesh axis runs over, the one named last changes fastest.
Arguments:
- hidden_in: bfloat16 [16384, 2048], P(('dp', 'mp')), may hold values from -6 to 6
- attn_gain: bfloat16 [2048], P('dp'), may hold values from 0.25 to 1.75
- w_query: bfloat16 [2048, 2048], P('dp', 'mp'), may hold values from -0.125 to 0.125
- key_projection: bfloat16 [2048, 1024], P('dp', 'mp'), may hold values from -0.125 to 0.125
- value_projection: bfloat16 [2048, 1024], P('dp', 'mp'), may hold values from -0.125 to 0.125
- query_gain: bfloat16 [128], replicated, may hold values from 1 to 2
- key_gain: bfloat16 [128], replicated, may hold values from 0.796875 to 1.59375
- w_out: bfloat16 [2048, 2048], P('mp', 'dp'), may hold values from -1 to 1
- mlp_gain: bfloat16 [2048], P('dp'), may hold values from 0.25 to 1.75
- w_gate: bfloat16 [2048, 6144], P('dp', 'mp'), may hold values from -0.125 to 0.125
- w_up: bfloat16 [2048, 6144], P('dp', 'mp'), may hold values from -0.125 to 0.125
- w_down: bfloat16 [6144, 2048], P('mp', 'dp'), may hold values from -0.078125 to 0.078125
- piece_start: int32 [8, 2], P('dp'), may hold values from 0 to 1792, as said below
- out_grad: bfloat16 [16384, 2048], P(('dp', 'mp')), may hold values from -6 to 6
Outputs:
- block_out: bfloat16 [16384, 2048], P(('dp', 'mp'))
- in_grad: float32 [16384, 2048], P(('dp', 'mp'))
- attn_gain_grad: float32 [2048], P('dp')
- w_query_grad: float32 [2048, 2048], P('dp', 'mp')
- w_key_grad: float32 [2048, 1024], P('dp', 'mp')
- w_value_grad: float32 [2048, 1024], P('dp', 'mp')
- query_gain_grad: float32 [128], replicated
- key_gain_grad: float32 [128], replicated
- w_out_grad: float32 [2048, 2048], P('mp', 'dp')
- mlp_gain_grad: float32 [2048], P('dp')
- w_gate_grad: float32 [2048, 6144], P('dp', 'mp')
- w_up_grad: float32 [2048, 6144], P('dp', 'mp')
- w_down_grad: float32 [6144, 2048], P('mp', 'dp')
The draws below stay inside these ranges and needn't reach their ends.
Inputs may be any that keep to these rules, and one draw needn't show every extreme that they name: `piece_start`: pieces of 256 tokens in order: piece p of a sequence starts between p * 1024 and (p + 1) * 1024 - 256; the first sequence's first piece starts at 0 and the last sequence's last piece ends at its last token.
All inputs are finite; a program needn't handle non-finite values.
Results may differ from the reference program's by a relative error of at most 0.022.
Values may be sent and summed in bfloat16 or wider, within the bound.
A program may use at most 320 MiB of HBM per device.

```python
import jax
import jax.numpy as jnp
from jax import lax

MODEL_WIDTH = 2048
QUERY_HEADS = 16
KEY_VALUE_HEADS = 8
HEAD_SIZE = 128
FF = 6144
SEQUENCE_TOKENS = 2048
PIECE = 256
QBLK = 512
SEQS = 8
TOKENS = 16384
PIECES = 2


def draw_piece_start(key, part):
    slot_size = SEQUENCE_TOKENS // PIECES
    offsets = jax.random.randint(jax.random.fold_in(key, 11), (SEQS, PIECES), 0, slot_size - PIECE + 1)
    offsets = offsets.at[0, 0].set(0)
    offsets = offsets.at[SEQS - 1, PIECES - 1].set(slot_size - PIECE)
    bases = jnp.arange(PIECES, dtype=jnp.int32)[None, :] * slot_size
    return (bases + offsets).astype(jnp.int32)


def block_levels(key, extent, pieces, smallest, high):
    def one(dim, parts):
        draws = jax.random.uniform(jax.random.fold_in(jax.random.fold_in(key, 6), dim), (parts,), jnp.float32, smallest / len(pieces), high / len(pieces))
        return jnp.repeat(jnp.exp(draws), extent[dim] // parts).reshape((-1,) + (1,) * (len(extent) - dim - 1))

    gain = one(*pieces[0])
    for cut in pieces[1:]:
        gain = gain * one(*cut)
    return gain


def noise(rng, extent, deviation, bound, cuts=(), kind=jnp.bfloat16):
    array = deviation * jax.random.normal(rng, extent, jnp.float32)
    if cuts:
        array = array * block_levels(rng, extent, cuts, -0.22, 0.18)
    return jnp.clip(array, -bound, bound).astype(kind)


def setup_inputs(seed: int = 0) -> dict:
    streams_of = jax.random.split(jax.random.key(seed), 15)
    return {
        "hidden_in": noise(streams_of[0], (TOKENS, MODEL_WIDTH), 1.0, 6.0, ((0, 32),)),
        "attn_gain": jnp.clip(1.0 + 0.15 * jax.random.normal(streams_of[1], (MODEL_WIDTH,), jnp.float32), 0.25, 1.75).astype(jnp.bfloat16),
        "w_query": noise(streams_of[2], (MODEL_WIDTH, QUERY_HEADS * HEAD_SIZE), MODEL_WIDTH ** -0.5, 0.125, ((0, 8), (1, 4))),
        "key_projection": noise(streams_of[3], (MODEL_WIDTH, KEY_VALUE_HEADS * HEAD_SIZE), MODEL_WIDTH ** -0.5, 0.125, ((0, 8), (1, 4))),
        "value_projection": noise(streams_of[4], (MODEL_WIDTH, KEY_VALUE_HEADS * HEAD_SIZE), MODEL_WIDTH ** -0.5, 0.125, ((0, 8), (1, 4))),
        "query_gain": jnp.clip(jax.random.uniform(streams_of[5], (HEAD_SIZE,), jnp.float32, 1.0, 2.0), 1.0, 2.0).astype(jnp.bfloat16),
        "key_gain": jnp.clip(jax.random.uniform(streams_of[6], (HEAD_SIZE,), jnp.float32, 0.796875, 1.59375), 0.796875, 1.59375).astype(jnp.bfloat16),
        "w_out": noise(streams_of[7], (QUERY_HEADS * HEAD_SIZE, MODEL_WIDTH), (QUERY_HEADS * HEAD_SIZE // 64) ** -0.5, 1.0, ((0, 4), (1, 8))),
        "mlp_gain": jnp.clip(1.0 + 0.15 * jax.random.normal(streams_of[8], (MODEL_WIDTH,), jnp.float32), 0.25, 1.75).astype(jnp.bfloat16),
        "w_gate": noise(streams_of[9], (MODEL_WIDTH, FF), MODEL_WIDTH ** -0.5, 0.125, ((0, 8), (1, 4))),
        "w_up": noise(streams_of[10], (MODEL_WIDTH, FF), MODEL_WIDTH ** -0.5, 0.125, ((0, 8), (1, 4))),
        "w_down": noise(streams_of[11], (FF, MODEL_WIDTH), FF ** -0.5, 0.078125, ((0, 4), (1, 8))),
        "piece_start": draw_piece_start(jax.random.fold_in(streams_of[14], 71), 0),
        "out_grad": noise(streams_of[13], (TOKENS, MODEL_WIDTH), 1.0, 6.0, ((0, 32),)),
    }


EPS = 1e-06
THETA = 1000000.0

@jax.custom_vjp
def lower_precision(v):
    return lax.optimization_barrier(v.astype(jnp.bfloat16)).astype(jnp.float32)

@jax.custom_vjp
def lower_precision_backward(v):
    return v

def low_keep(v):
    return (lower_precision(v), None)

def low_pass(kept, grad):
    return (grad,)

def back_keep(v):
    return (v, None)

def back_low(kept, grad):
    return (lower_precision(grad),)
lower_precision.defvjp(low_keep, low_pass)
lower_precision_backward.defvjp(back_keep, back_low)

def matrix_product(left, right):
    return jnp.dot(left, right, precision=lax.Precision.HIGHEST)

def normalized(values):
    return values * lax.rsqrt(lax.optimization_barrier(jnp.mean(values * values, axis=-1, keepdims=True)) + EPS)

def rotary_tables(seq_len, width):
    steps = jnp.arange(width // 2, dtype=jnp.float32)
    inverse = THETA ** (-(2.0 * steps) / width)
    angles = jnp.arange(seq_len, dtype=jnp.float32)[:, None] * inverse[None, :]
    return (jnp.cos(angles), jnp.sin(angles))

def rotate(heads, cosine, sine):
    half = heads.shape[-1] // 2
    first = heads[..., :half]
    second = heads[..., half:]
    cos_part = cosine[:, None, :]
    sin_part = sine[:, None, :]
    return jnp.concatenate([first * cos_part - second * sin_part, second * cos_part + first * sin_part], axis=-1)

def norm_rope(heads, weight, cosine, sine):
    return rotate(normalized(heads) * weight, cosine, sine)

def piece_labels(starts, seq_len):
    spots = jnp.arange(seq_len, dtype=jnp.int32)
    inside = (spots[None, :] >= starts[:, None]) & (spots[None, :] < starts[:, None] + PIECE)
    numbers = jnp.arange(1, starts.shape[0] + 1, dtype=jnp.int32)
    return lax.optimization_barrier(jnp.sum(jnp.where(inside, numbers[:, None], 0), axis=0)).astype(jnp.int32)

def visible(first_row, labels):
    seq_len = labels.shape[0]
    row_ids = first_row + jnp.arange(QBLK, dtype=jnp.int32)
    row_labels = lax.dynamic_slice_in_dim(labels, first_row, QBLK, 0)
    col_ids = jnp.arange(seq_len, dtype=jnp.int32)
    causal = col_ids[None, :] <= row_ids[:, None]
    same_piece = (row_labels[:, None] == labels[None, :]) & (row_labels[:, None] > 0)
    return causal | same_piece

def attend(query_heads, key, value_heads, labels):
    group_count = QUERY_HEADS // KEY_VALUE_HEADS
    grouped_heads = query_heads.reshape(SEQUENCE_TOKENS, KEY_VALUE_HEADS, group_count, HEAD_SIZE)
    score_scale = HEAD_SIZE ** (-0.5)

    def block(block_index):
        first_row = (block_index * QBLK).astype(jnp.int32)
        query_rows = lax.dynamic_slice_in_dim(grouped_heads, first_row, QBLK, 0)
        scores = jnp.einsum('qhgd,khd->hgqk', query_rows, key, precision=lax.Precision.HIGHEST) * score_scale
        scores = lower_precision_backward(scores)
        shown = visible(first_row, labels)
        scores = jnp.where(shown[None, None], scores, -1e+30)
        largest = lax.optimization_barrier(jnp.max(scores, axis=-1, keepdims=True))
        expo = jnp.exp(scores - largest)
        share = lower_precision(expo / lax.optimization_barrier(jnp.sum(expo, axis=-1, keepdims=True)))
        return jnp.einsum('hgqk,khd->qhgd', share, value_heads, precision=lax.Precision.HIGHEST)
    outs = lax.map(jax.checkpoint(block), jnp.arange(SEQUENCE_TOKENS // QBLK, dtype=jnp.int32))
    return outs.reshape(SEQUENCE_TOKENS, QUERY_HEADS * HEAD_SIZE)

def layer(rows_in, gain_one, query_w, key_matrix, value_matrix, query_g, key_g, out_w, gain_two, gate_w, up_w, down_w, labels):
    cosine, sine = rotary_tables(SEQUENCE_TOKENS, HEAD_SIZE)
    hidden_first = lower_precision(normalized(rows_in) * gain_one)
    query_raw = lower_precision_backward(matrix_product(hidden_first, query_w)).reshape(SEQUENCE_TOKENS, QUERY_HEADS, HEAD_SIZE)
    key_unrotated = lower_precision_backward(matrix_product(hidden_first, key_matrix)).reshape(SEQUENCE_TOKENS, KEY_VALUE_HEADS, HEAD_SIZE)
    value_heads = lower_precision(lower_precision_backward(matrix_product(hidden_first, value_matrix))).reshape(SEQUENCE_TOKENS, KEY_VALUE_HEADS, HEAD_SIZE)
    query_heads = lower_precision(norm_rope(query_raw, query_g, cosine, sine))
    key = lower_precision(norm_rope(key_unrotated, key_g, cosine, sine))
    attended = lower_precision(lower_precision_backward(attend(query_heads, key, value_heads, labels)))
    x_two = rows_in + lower_precision_backward(matrix_product(attended, out_w))
    h_two = lower_precision(normalized(x_two) * gain_two)
    gate = lower_precision_backward(matrix_product(h_two, gate_w))
    up_val = lower_precision_backward(matrix_product(h_two, up_w))
    hidden = lower_precision(jax.nn.silu(gate) * up_val)
    return x_two + lower_precision_backward(matrix_product(hidden, down_w))

def reference(hidden_in, attn_gain, w_query, key_projection, value_projection, query_gain, key_gain, w_out, mlp_gain, w_gate, w_up, w_down, piece_start, out_grad):
    params = tuple((item.astype(jnp.float32) for item in (attn_gain, w_query, key_projection, value_projection, query_gain, key_gain, w_out, mlp_gain, w_gate, w_up, w_down)))
    seq_rows = hidden_in.astype(jnp.float32).reshape(SEQS, SEQUENCE_TOKENS, MODEL_WIDTH)
    seq_cot = out_grad.astype(jnp.float32).reshape(SEQS, SEQUENCE_TOKENS, MODEL_WIDTH)

    def one_seq(totals, item):
        rows_in, cotangent, starts = item
        labels = piece_labels(starts, SEQUENCE_TOKENS)

        def forward(values, *weights):
            return layer(values, *weights, labels)
        result, pullback = jax.vjp(forward, rows_in, *params)
        grads = pullback(cotangent)
        totals = tuple((total + grad for total, grad in zip(totals, grads[1:])))
        return (totals, (result.astype(jnp.bfloat16), grads[0]))
    init = tuple((jnp.zeros(item.shape, jnp.float32) for item in params))
    totals, (results, input_grads) = lax.scan(one_seq, init, (seq_rows, seq_cot, piece_start))
    return (results.reshape(TOKENS, MODEL_WIDTH), input_grads.reshape(TOKENS, MODEL_WIDTH), totals[0], totals[1], totals[2], totals[3], totals[4], totals[5], totals[6], totals[7], totals[8], totals[9], totals[10])
```

```python
import functools

import jax
import jax.numpy as jnp
from jax import lax
from jax.experimental import pallas as pl
from jax.experimental.pallas import tpu as pltpu
from jax.sharding import PartitionSpec as P

PIECE = 256
EPS = 1e-06
THETA = 1000000.0
LOG2E = 1.4426950408889634
F32 = jnp.float32
BF16 = jnp.bfloat16


def dot(left, right):
    return jnp.dot(left, right, preferred_element_type=F32)


def dot_tl(left, right):
    return lax.dot_general(left, right, (((0,), (0,)), ((), ())), preferred_element_type=F32)


def dot_tr(left, right):
    return lax.dot_general(left, right, (((1,), (1,)), ((), ())), preferred_element_type=F32)


def inverse_rms(values):
    return lax.rsqrt(jnp.mean(values * values, axis=-1, keepdims=True) + EPS)


def rotary_tables(seq_len, width):
    steps = jnp.arange(width // 2, dtype=F32)
    inverse = THETA ** (-(2.0 * steps) / width)
    angles = jnp.arange(seq_len, dtype=F32)[:, None] * inverse[None, :]
    cosine, sine = jnp.cos(angles), jnp.sin(angles)
    return (
        jnp.concatenate([cosine, cosine], axis=-1),
        jnp.concatenate([-sine, sine], axis=-1),
    )


def hop(array, shift):
    size = lax.axis_size("mp")
    return lax.ppermute(array, "mp", [(i, (i + shift) % size) for i in range(size)])


def ring_gather(array):
    items = [array]
    for _ in range(lax.axis_size("mp") - 1):
        items.append(hop(items[-1], 1))
    return items


def ring_scatter(partial):
    size = lax.axis_size("mp")
    total = partial(1 % size)
    for k in list(range(2, size)) + [0]:
        arrived = hop(total.astype(BF16), 1).astype(F32)
        total = arrived + partial(k)
    return total


def norm_rope(raw, gain, cosine, sine):
    normed = raw * inverse_rms(raw)
    scaled = normed * gain
    return scaled * cosine + pltpu.roll(scaled, raw.shape[-1] // 2, 1) * sine


def norm_rope_back(raw, gain, cosine, sine, grad):
    inv = inverse_rms(raw)
    normed = raw * inv
    turned = grad * cosine + pltpu.roll(grad * sine, raw.shape[-1] // 2, 1)
    gain_part = jnp.sum(turned * normed, axis=0, keepdims=True)
    inner = turned * gain
    back = (inner - normed * jnp.mean(inner * normed, axis=-1, keepdims=True)) * inv
    return back, gain_part


def labels_of(starts, spots, nothing):
    result = jnp.full(spots.shape, nothing, jnp.int32)
    for p, start in enumerate(starts):
        result = jnp.where((spots >= start) & (spots < start + PIECE), p + 1, result)
    return result


def masked(scores, row_first, col_first, starts, group):
    rows, cols = scores.shape
    block = rows // group
    spots = row_first + lax.rem(lax.broadcasted_iota(jnp.int32, (rows, 1), 0), block)
    keys = col_first + lax.broadcasted_iota(jnp.int32, (1, cols), 1)
    shown = (keys <= spots) | (labels_of(starts, spots, 0) == labels_of(starts, keys, -1))
    return shown


def crosses(starts, edge):
    hit = (starts[0] < edge) & (starts[0] + PIECE > edge)
    for start in starts[1:]:
        hit = hit | ((start < edge) & (start + PIECE > edge))
    return hit


def stack_heads(array, group, width):
    return jnp.concatenate([array[:, g * width : (g + 1) * width] for g in range(group)], axis=0)


def attend_kernel(chunks, group, pieces, place, piece_ref, raw_q, raw_k, value, cosine, sine,
                  gain_q, gain_k, out, log_out, key_all, value_all):
    rows = raw_q.shape[0]
    width = raw_k.shape[1]
    scale = width ** (-0.5) * LOG2E
    step = pl.program_id(1)
    starts = [piece_ref[p] for p in range(pieces)]

    @pl.when(step == 0)
    def _():
        def fill(c, carry):
            first = pl.multiple_of(place[c] * rows, rows)
            here = pl.ds(first, rows)
            there = pl.ds(pl.multiple_of(c * rows, rows), rows)
            key_all[here, :] = norm_rope(
                raw_k[there, :], gain_k[...], cosine[here, :], sine[here, :]
            ).astype(BF16)
            value_all[here, :] = value[there, :]
            return carry

        lax.fori_loop(0, chunks, fill, 0)

    mine = place[step]
    first = pl.multiple_of(mine * rows, rows)
    cos_here = cosine[pl.ds(first, rows), :]
    sin_here = sine[pl.ds(first, rows), :]
    query = jnp.concatenate(
        [
            norm_rope(raw_q[:, g * width : (g + 1) * width], gain_q[...], cos_here, sin_here)
            for g in range(group)
        ],
        axis=0,
    ).astype(BF16)

    def part(block, mask, carry):
        total, result = carry
        at = pl.multiple_of(block * rows, rows)
        keys = key_all[pl.ds(at, rows), :]
        expo = jnp.exp2(dot_tr(query, keys) * scale)
        if mask:
            expo = jnp.where(masked(expo, first, at, starts, group), expo, 0.0)
        total = total + jnp.sum(expo, axis=-1, keepdims=True)
        result = result + dot(expo.astype(BF16), value_all[pl.ds(at, rows), :])
        return total, result

    carry = (
        jnp.zeros((rows * group, 1), F32),
        jnp.zeros((rows * group, width), F32),
    )
    carry = lax.fori_loop(0, mine, lambda b, c: part(b, False, c), carry)
    ends = jnp.where((mine + 1 < chunks) & crosses(starts, first + rows), mine + 2, mine + 1)
    total, result = lax.fori_loop(mine, ends, lambda b, c: part(b, True, c), carry)
    result = result / total
    log_norm = jnp.log2(total)
    for g in range(group):
        part_rows = slice(g * rows, (g + 1) * rows)
        out[:, g * width : (g + 1) * width] = result[part_rows].astype(BF16)
        log_out[:, g * width : (g + 1) * width] = jnp.broadcast_to(
            log_norm[part_rows], (rows, width)
        )


def attend_back_kernel(chunks, group, pieces, place, piece_ref, raw_q, raw_k, value, cosine, sine,
                       gain_q, gain_k, attended, log_norm, grad, query_grad, key_grad, value_grad,
                       gain_q_grad, gain_k_grad, key_all, value_all, key_sum, value_sum):
    rows = raw_q.shape[0]
    width = raw_k.shape[1]
    plain = width ** (-0.5)
    scale = plain * LOG2E
    head, step = pl.program_id(0), pl.program_id(1)
    starts = [piece_ref[p] for p in range(pieces)]

    @pl.when((head == 0) & (step == 0))
    def _():
        gain_q_grad[...] = jnp.zeros_like(gain_q_grad)
        gain_k_grad[...] = jnp.zeros_like(gain_k_grad)

    @pl.when(step == 0)
    def _():
        key_sum[...] = jnp.zeros_like(key_sum)
        value_sum[...] = jnp.zeros_like(value_sum)

        def fill(c, carry):
            here = pl.ds(pl.multiple_of(place[c] * rows, rows), rows)
            there = pl.ds(pl.multiple_of(c * rows, rows), rows)
            key_all[here, :] = norm_rope(
                raw_k[there, :], gain_k[...], cosine[here, :], sine[here, :]
            ).astype(BF16)
            value_all[here, :] = value[there, :]
            return carry

        lax.fori_loop(0, chunks, fill, 0)

    mine = place[step]
    first = pl.multiple_of(mine * rows, rows)
    cos_here = cosine[pl.ds(first, rows), :]
    sin_here = sine[pl.ds(first, rows), :]
    query = jnp.concatenate(
        [
            norm_rope(raw_q[:, g * width : (g + 1) * width], gain_q[...], cos_here, sin_here)
            for g in range(group)
        ],
        axis=0,
    ).astype(BF16)
    grads = stack_heads(grad[...], group, width)
    norms = jnp.concatenate([log_norm[:, g * width : g * width + 1] for g in range(group)], axis=0)
    dots = jnp.sum(
        grads.astype(F32) * stack_heads(attended[...], group, width).astype(F32),
        axis=-1,
        keepdims=True,
    )

    def part(block, mask, total):
        at = pl.multiple_of(block * rows, rows)
        here = pl.ds(at, rows)
        keys = key_all[here, :]
        share = jnp.exp2(dot_tr(query, keys) * scale - norms)
        if mask:
            share = jnp.where(masked(share, first, at, starts, group), share, 0.0)
        share_grad = dot_tr(grads, value_all[here, :])
        score_grad = (share * (share_grad - dots)).astype(BF16)
        value_sum[here, :] += dot_tl(share.astype(BF16), grads)
        key_sum[here, :] += dot_tl(score_grad, query)
        return total + dot(score_grad, keys)

    total = jnp.zeros((rows * group, width), F32)
    total = lax.fori_loop(0, mine, lambda b, c: part(b, False, c), total)
    ends = jnp.where((mine + 1 < chunks) & crosses(starts, first + rows), mine + 2, mine + 1)
    total = lax.fori_loop(mine, ends, lambda b, c: part(b, True, c), total)
    for g in range(group):
        columns = slice(g * width, (g + 1) * width)
        back, gain_part = norm_rope_back(
            raw_q[:, columns],
            gain_q[...],
            cos_here,
            sin_here,
            total[g * rows : (g + 1) * rows] * plain,
        )
        query_grad[:, columns] = back.astype(BF16)
        gain_q_grad[...] += gain_part

    @pl.when(step == chunks - 1)
    def _():
        def drain(c, carry):
            here = pl.ds(pl.multiple_of(place[c] * rows, rows), rows)
            there = pl.ds(pl.multiple_of(c * rows, rows), rows)
            back, gain_part = norm_rope_back(
                raw_k[there, :], gain_k[...], cosine[here, :], sine[here, :],
                key_sum[here, :] * plain,
            )
            key_grad[there, :] = back.astype(BF16)
            value_grad[there, :] = value_sum[here, :].astype(BF16)
            gain_k_grad[...] += gain_part
            return carry

        lax.fori_loop(0, chunks, drain, 0)


def attention_specs(rows, seq_len, group, width):
    by_chunk = pl.BlockSpec((rows, group * width), lambda h, c, *_: (c, h))
    by_head = pl.BlockSpec((seq_len, width), lambda h, c, *_: (0, h))
    table = pl.BlockSpec((seq_len, width), lambda h, c, *_: (0, 0))
    gain = pl.BlockSpec((1, width), lambda h, c, *_: (0, 0))
    return by_chunk, by_head, table, gain


def attend(place, starts, raw_q, raw_k, value, tables, gain_q, gain_k):
    chunks, width = place.shape[0], gain_q.shape[1]
    seq_len = raw_q.shape[0]
    rows, kv_heads = seq_len // chunks, raw_k.shape[1] // width
    group = raw_q.shape[1] // raw_k.shape[1]
    by_chunk, by_head, table, gain = attention_specs(rows, seq_len, group, width)
    return pl.pallas_call(
        functools.partial(attend_kernel, chunks, group, starts.shape[0]),
        grid_spec=pltpu.PrefetchScalarGridSpec(
            num_scalar_prefetch=2,
            grid=(kv_heads, chunks),
            in_specs=[by_chunk, by_head, by_head, table, table, gain, gain],
            out_specs=[by_chunk, by_chunk],
            scratch_shapes=[pltpu.VMEM((seq_len, width), BF16)] * 2,
        ),
        out_shape=[
            jax.ShapeDtypeStruct(raw_q.shape, BF16),
            jax.ShapeDtypeStruct(raw_q.shape, F32),
        ],
        compiler_params=pltpu.CompilerParams(vmem_limit_bytes=48 << 20),
        cost_estimate=pl.CostEstimate(
            flops=2 * seq_len * seq_len * raw_q.shape[1],
            bytes_accessed=14 * raw_q.size,
            transcendentals=seq_len * seq_len,
        ),
        name="attend",
    )(place, starts, raw_q, raw_k, value, *tables, gain_q, gain_k)


def attend_back(place, starts, raw_q, raw_k, value, tables, gain_q, gain_k, attended, log_norm,
                grad):
    chunks, width = place.shape[0], gain_q.shape[1]
    seq_len = raw_q.shape[0]
    rows, kv_heads = seq_len // chunks, raw_k.shape[1] // width
    group = raw_q.shape[1] // raw_k.shape[1]
    by_chunk, by_head, table, gain = attention_specs(rows, seq_len, group, width)
    return pl.pallas_call(
        functools.partial(attend_back_kernel, chunks, group, starts.shape[0]),
        grid_spec=pltpu.PrefetchScalarGridSpec(
            num_scalar_prefetch=2,
            grid=(kv_heads, chunks),
            in_specs=[by_chunk, by_head, by_head, table, table, gain, gain] + [by_chunk] * 3,
            out_specs=[by_chunk, by_head, by_head, gain, gain],
            scratch_shapes=[pltpu.VMEM((seq_len, width), BF16)] * 2
            + [pltpu.VMEM((seq_len, width), F32)] * 2,
        ),
        out_shape=[
            jax.ShapeDtypeStruct(raw_q.shape, BF16),
            jax.ShapeDtypeStruct(raw_k.shape, BF16),
            jax.ShapeDtypeStruct(raw_k.shape, BF16),
            jax.ShapeDtypeStruct((1, width), F32),
            jax.ShapeDtypeStruct((1, width), F32),
        ],
        compiler_params=pltpu.CompilerParams(vmem_limit_bytes=56 << 20),
        cost_estimate=pl.CostEstimate(
            flops=6 * seq_len * seq_len * raw_q.shape[1],
            bytes_accessed=18 * raw_q.size,
            transcendentals=seq_len * seq_len,
        ),
        name="attend_back",
    )(place, starts, raw_q, raw_k, value, *tables, gain_q, gain_k, attended, log_norm, grad)


def rms_back(values, grad):
    inv = inverse_rms(values)
    normed = values * inv
    return (grad - normed * jnp.mean(grad * normed, axis=-1, keepdims=True)) * inv


def gain_sums(wide, narrow):
    size, data = lax.axis_size("mp"), lax.axis_size("dp")
    vector = jnp.concatenate([wide.reshape(-1), narrow.reshape(-1)])
    total = vector
    for k in range(1, size):
        total = total + hop(vector, k)
    count = wide.shape[0]
    spread = total[: wide.size].reshape(count, data, -1)
    small = total[wide.size :]
    me = lax.axis_index("dp")

    def slice_for(device):
        cut = lax.dynamic_index_in_dim(spread, device, 1, keepdims=False)
        return jnp.concatenate([cut.reshape(-1), small])

    result = slice_for(me)
    for k in range(1, data):
        sent = slice_for(lax.rem(me + k, data))
        result = result + lax.ppermute(sent, "dp", [(i, (i + k) % data) for i in range(data)])
    cut_size = wide.size // data
    return result[:cut_size].reshape(count, -1), result[cut_size:].reshape(narrow.shape)


def shards(hidden_in, attn_gain, w_query, key_projection, value_projection, query_gain, key_gain,
           w_out, mlp_gain, w_gate, w_up, w_down, piece_start, out_grad):
    tok_rows = hidden_in.shape[0]
    size = lax.axis_size("mp")
    seq_len = tok_rows * size
    me = lax.axis_index("mp")
    head_dim = query_gain.shape[0]
    q_width, kv_width = w_query.shape[1], key_projection.shape[1]
    place = lax.rem(me - jnp.arange(size, dtype=jnp.int32) + size, size)
    starts = piece_start[0]
    tables = rotary_tables(seq_len, head_dim)
    gain_q = query_gain.astype(F32)[None]
    gain_k = key_gain.astype(F32)[None]

    gains = lax.all_gather(jnp.stack([attn_gain, mlp_gain], axis=0), "dp", axis=1, tiled=True)
    gain_one, gain_two = gains[0].astype(F32), gains[1].astype(F32)
    qkv_all = lax.all_gather(
        jnp.concatenate([w_query, key_projection, value_projection], axis=1),
        "dp", axis=0, tiled=True,
    )

    x_own = hidden_in.astype(F32)
    x_items = ring_gather(hidden_in)
    out_items = [w_out]
    for _ in range(size - 1):
        out_items.append(hop(out_items[-1], -1))
    out_all = lax.all_gather(jnp.concatenate(out_items, axis=0), "dp", axis=1, tiled=True)
    gate_all = lax.all_gather(w_gate, "dp", axis=0, tiled=True)
    up_all = lax.all_gather(w_up, "dp", axis=0, tiled=True)
    down_all = lax.all_gather(w_down, "dp", axis=1, tiled=True)

    h_one_items, raw_items = [], []
    for item in x_items:
        rows = item.astype(F32)
        h_one = (rows * inverse_rms(rows) * gain_one).astype(BF16)
        h_one_items.append(h_one)
        raw_items.append(dot(h_one, qkv_all))
    h_one_all = jnp.concatenate(h_one_items, axis=0)
    raw_q = jnp.concatenate([item[:, :q_width] for item in raw_items], axis=0)
    raw_k = jnp.concatenate([item[:, q_width : q_width + kv_width] for item in raw_items], axis=0)
    value = jnp.concatenate(
        [item[:, q_width + kv_width :].astype(BF16) for item in raw_items], axis=0
    )
    attended, log_norm = attend(place, starts, raw_q, raw_k, value, tables, gain_q, gain_k)

    cot_items = ring_gather(out_grad)

    def chunk(array, k):
        return array[k * tok_rows : (k + 1) * tok_rows]

    own_items = [chunk(attended, 0)] + [hop(chunk(attended, k), -k) for k in range(1, size)]
    attended_own = jnp.concatenate(own_items, axis=1)
    x_two = x_own + dot(attended_own, out_all)
    normed_two = x_two * inverse_rms(x_two)
    h_two = (normed_two * gain_two).astype(BF16)
    h_two_items = ring_gather(h_two)

    gates, ups, hiddens = [], [], []
    for item in h_two_items:
        gate = dot(item, gate_all)
        up_val = dot(item, up_all)
        gates.append(gate)
        ups.append(up_val)
        hiddens.append((gate * jax.nn.sigmoid(gate) * up_val).astype(BF16))

    gate_lows, up_lows = [None] * size, [None] * size
    for k in list(range(1, size)) + [0]:
        hidden_grad = dot_tr(cot_items[k], down_all)
        sig = jax.nn.sigmoid(gates[k])
        gate_lows[k] = (
            hidden_grad * ups[k] * (sig * (1.0 + gates[k] * (1.0 - sig)))
        ).astype(BF16)
        up_lows[k] = (hidden_grad * (gates[k] * sig)).astype(BF16)

    h_two_grad = ring_scatter(
        lambda k: dot_tr(gate_lows[k], gate_all) + dot_tr(up_lows[k], up_all)
    )
    mlp_rows = ring_scatter(lambda k: dot(hiddens[k], down_all))
    block_out = (x_two + mlp_rows.astype(BF16).astype(F32)).astype(BF16)

    h_two_all = jnp.concatenate(h_two_items, axis=0)
    cot_all = jnp.concatenate(cot_items, axis=0)
    down_wgrad = dot_tl(jnp.concatenate(hiddens, axis=0), cot_all).astype(BF16)
    gate_wgrad = dot_tl(h_two_all, jnp.concatenate(gate_lows, axis=0)).astype(BF16)
    up_wgrad = dot_tl(h_two_all, jnp.concatenate(up_lows, axis=0)).astype(BF16)

    gain_two_part = jnp.sum(h_two_grad * normed_two, axis=0)
    x_two_grad = out_grad.astype(F32) + rms_back(x_two, h_two_grad * gain_two)
    attn_grad = x_two_grad.astype(BF16)
    attended_grad_own = dot_tr(attn_grad, out_all).astype(BF16)
    grad_items = [attended_grad_own[:, :q_width]] + [
        hop(attended_grad_own[:, k * q_width : (k + 1) * q_width], k) for k in range(1, size)
    ]
    attended_grad = jnp.concatenate(grad_items, axis=0)
    out_wgrad = dot_tl(attended_own, attn_grad).astype(BF16)

    query_grad, key_grad, value_grad, gain_q_part, gain_k_part = attend_back(
        place, starts, raw_q, raw_k, value, tables, gain_q, gain_k, attended, log_norm,
        attended_grad,
    )
    qkv_grad = jnp.concatenate([query_grad, key_grad, value_grad], axis=1)
    h_one_grad = ring_scatter(lambda k: dot_tr(chunk(qkv_grad, k), qkv_all))
    qkv_wgrad = dot_tl(h_one_all, qkv_grad).astype(BF16)

    normed_one = x_own * inverse_rms(x_own)
    gain_one_part = jnp.sum(h_one_grad * normed_one, axis=0)
    in_grad = x_two_grad + rms_back(x_own, h_one_grad * gain_one)

    def scatter(array, dim):
        return lax.psum_scatter(array, "dp", scatter_dimension=dim, tiled=True)

    down_sum = scatter(down_wgrad, 1).astype(F32)
    gate_sum = scatter(gate_wgrad, 0).astype(F32)
    up_sum = scatter(up_wgrad, 0).astype(F32)
    out_cut = scatter(out_wgrad, 1)
    block = w_out.shape[0]
    out_sum = out_cut[:block].astype(F32)
    for k in range(1, size):
        out_sum = out_sum + hop(out_cut[k * block : (k + 1) * block], k).astype(F32)
    qkv_sum = scatter(qkv_wgrad, 0).astype(F32)

    wide, narrow = gain_sums(
        jnp.stack([gain_one_part, gain_two_part]),
        jnp.concatenate([gain_q_part, gain_k_part], axis=0),
    )
    return (
        block_out, in_grad, wide[0],
        qkv_sum[:, :q_width], qkv_sum[:, q_width : q_width + kv_width],
        qkv_sum[:, q_width + kv_width :],
        narrow[0], narrow[1], out_sum, wide[1], gate_sum, up_sum, down_sum,
    )


def solution(mesh):
    both = P(("dp", "mp"), None)
    weight, turned = P("dp", "mp"), P("mp", "dp")
    return jax.shard_map(
        shards,
        mesh=mesh,
        in_specs=(
            both, P("dp"), weight, weight, weight, P(), P(), turned, P("dp"), weight, weight,
            turned, P("dp", None), both,
        ),
        out_specs=(
            both, both, P("dp"), weight, weight, weight, P(), P(), turned, P("dp"), weight, weight,
            turned,
        ),
        check_vma=False,
    )
```

```python
import functools

import jax
import jax.numpy as jnp
from jax import lax
from jax.experimental import pallas as pl
from jax.experimental.pallas import tpu as pltpu
from jax.sharding import PartitionSpec as P


PIECE = 256
EPS = 1e-06
THETA = 1000000.0
LOG2E = 1.4426950408889634
F32 = jnp.float32
BF16 = jnp.bfloat16


def dot(left, right):
    return jnp.dot(left, right, preferred_element_type=F32)


def dot_tl(left, right):
    return lax.dot_general(left, right, (((0,), (0,)), ((), ())), preferred_element_type=F32)


def dot_tr(left, right):
    return lax.dot_general(left, right, (((1,), (1,)), ((), ())), preferred_element_type=F32)


def inverse_rms(values):
    return lax.rsqrt(jnp.mean(values * values, axis=-1, keepdims=True) + EPS)


def rotary_tables(seq_len, width):
    steps = jnp.arange(width // 2, dtype=F32)
    inverse = THETA ** (-(2.0 * steps) / width)
    angles = jnp.arange(seq_len, dtype=F32)[:, None] * inverse[None, :]
    cosine, sine = jnp.cos(angles), jnp.sin(angles)
    return (
        jnp.concatenate([cosine, cosine], axis=-1),
        jnp.concatenate([-sine, sine], axis=-1),
    )


def hop(array, shift):
    size = lax.axis_size("mp")
    return lax.ppermute(array, "mp", [(i, (i + shift) % size) for i in range(size)])


def after(value, *others):
    return lax.optimization_barrier((value,) + others)[0]


def tied(*values):
    return lax.optimization_barrier(values)


def ring_gather(array):
    items = [array]
    for _ in range(lax.axis_size("mp") - 1):
        items.append(hop(items[-1], 1))
    return items


def norm_rope(raw, gain, cosine, sine):
    normed = raw * inverse_rms(raw)
    scaled = normed * gain
    return scaled * cosine + pltpu.roll(scaled, raw.shape[-1] // 2, 1) * sine


def norm_rope_back(raw, gain, cosine, sine, grad):
    inv = inverse_rms(raw)
    normed = raw * inv
    turned = grad * cosine + pltpu.roll(grad * sine, raw.shape[-1] // 2, 1)
    gain_part = jnp.sum(turned * normed, axis=0, keepdims=True)
    inner = turned * gain
    back = (inner - normed * jnp.mean(inner * normed, axis=-1, keepdims=True)) * inv
    return back, gain_part


def labels_of(starts, spots, nothing):
    result = jnp.full(spots.shape, nothing, jnp.int32)
    for p, start in enumerate(starts):
        result = jnp.where((spots >= start) & (spots < start + PIECE), p + 1, result)
    return result


def masked(scores, row_first, col_first, starts, group):
    rows, cols = scores.shape
    block = rows // group
    spots = row_first + lax.rem(lax.broadcasted_iota(jnp.int32, (rows, 1), 0), block)
    keys = col_first + lax.broadcasted_iota(jnp.int32, (1, cols), 1)
    shown = (keys <= spots) | (labels_of(starts, spots, 0) == labels_of(starts, keys, -1))
    return shown


def crosses(starts, edge):
    hit = (starts[0] < edge) & (starts[0] + PIECE > edge)
    for start in starts[1:]:
        hit = hit | ((start < edge) & (start + PIECE > edge))
    return hit


def stack_heads(array, group, width):
    return jnp.concatenate([array[:, g * width : (g + 1) * width] for g in range(group)], axis=0)


def attend_kernel(chunks, group, pieces, place, piece_ref, raw_q, raw_k, value, cosine, sine,
                  gain_q, gain_k, out, log_out, key_all, value_all):
    rows = raw_q.shape[0]
    width = raw_k.shape[1]
    scale = width ** (-0.5) * LOG2E
    step = pl.program_id(1)
    starts = [piece_ref[p] for p in range(pieces)]

    @pl.when(step == 0)
    def _():
        def fill(c, carry):
            first = pl.multiple_of(place[c] * rows, rows)
            here = pl.ds(first, rows)
            there = pl.ds(pl.multiple_of(c * rows, rows), rows)
            key_all[here, :] = norm_rope(
                raw_k[there, :], gain_k[...], cosine[here, :], sine[here, :]
            ).astype(BF16)
            value_all[here, :] = value[there, :]
            return carry

        lax.fori_loop(0, chunks, fill, 0)

    mine = place[step]
    first = pl.multiple_of(mine * rows, rows)
    cos_here = cosine[pl.ds(first, rows), :]
    sin_here = sine[pl.ds(first, rows), :]
    query = jnp.concatenate(
        [
            norm_rope(raw_q[:, g * width : (g + 1) * width], gain_q[...], cos_here, sin_here)
            for g in range(group)
        ],
        axis=0,
    ).astype(BF16)

    def part(block, mask, carry):
        total, result = carry
        at = pl.multiple_of(block * rows, rows)
        keys = key_all[pl.ds(at, rows), :]
        expo = jnp.exp2(dot_tr(query, keys) * scale)
        if mask:
            expo = jnp.where(masked(expo, first, at, starts, group), expo, 0.0)
        total = total + jnp.sum(expo, axis=-1, keepdims=True)
        result = result + dot(expo.astype(BF16), value_all[pl.ds(at, rows), :])
        return total, result

    carry = (
        jnp.zeros((rows * group, 1), F32),
        jnp.zeros((rows * group, width), F32),
    )
    carry = lax.fori_loop(0, mine, lambda b, c: part(b, False, c), carry)
    ends = jnp.where((mine + 1 < chunks) & crosses(starts, first + rows), mine + 2, mine + 1)
    total, result = lax.fori_loop(mine, ends, lambda b, c: part(b, True, c), carry)
    result = result / total
    log_norm = jnp.log2(total)
    for g in range(group):
        part_rows = slice(g * rows, (g + 1) * rows)
        out[:, g * width : (g + 1) * width] = result[part_rows].astype(BF16)
        log_out[:, g * width : (g + 1) * width] = jnp.broadcast_to(
            log_norm[part_rows], (rows, width)
        )


def attend_back_kernel(chunks, group, pieces, place, piece_ref, raw_q, raw_k, value, cosine, sine,
                       gain_q, gain_k, attended, log_norm, grad, query_grad, key_grad, value_grad,
                       gain_q_grad, gain_k_grad, key_all, value_all, key_sum, value_sum):
    rows = raw_q.shape[0]
    width = raw_k.shape[1]
    plain = width ** (-0.5)
    scale = plain * LOG2E
    head, step = pl.program_id(0), pl.program_id(1)
    starts = [piece_ref[p] for p in range(pieces)]

    @pl.when((head == 0) & (step == 0))
    def _():
        gain_q_grad[...] = jnp.zeros_like(gain_q_grad)
        gain_k_grad[...] = jnp.zeros_like(gain_k_grad)

    @pl.when(step == 0)
    def _():
        key_sum[...] = jnp.zeros_like(key_sum)
        value_sum[...] = jnp.zeros_like(value_sum)

        def fill(c, carry):
            here = pl.ds(pl.multiple_of(place[c] * rows, rows), rows)
            there = pl.ds(pl.multiple_of(c * rows, rows), rows)
            key_all[here, :] = norm_rope(
                raw_k[there, :], gain_k[...], cosine[here, :], sine[here, :]
            ).astype(BF16)
            value_all[here, :] = value[there, :]
            return carry

        lax.fori_loop(0, chunks, fill, 0)

    mine = place[step]
    first = pl.multiple_of(mine * rows, rows)
    cos_here = cosine[pl.ds(first, rows), :]
    sin_here = sine[pl.ds(first, rows), :]
    query = jnp.concatenate(
        [
            norm_rope(raw_q[:, g * width : (g + 1) * width], gain_q[...], cos_here, sin_here)
            for g in range(group)
        ],
        axis=0,
    ).astype(BF16)
    grads = stack_heads(grad[...], group, width)
    norms = jnp.concatenate([log_norm[:, g * width : g * width + 1] for g in range(group)], axis=0)
    dots = jnp.sum(
        grads.astype(F32) * stack_heads(attended[...], group, width).astype(F32),
        axis=-1,
        keepdims=True,
    )

    def part(block, mask, total):
        at = pl.multiple_of(block * rows, rows)
        here = pl.ds(at, rows)
        keys = key_all[here, :]
        share = jnp.exp2(dot_tr(query, keys) * scale - norms)
        if mask:
            share = jnp.where(masked(share, first, at, starts, group), share, 0.0)
        share_grad = dot_tr(grads, value_all[here, :])
        score_grad = (share * (share_grad - dots)).astype(BF16)
        value_sum[here, :] += dot_tl(share.astype(BF16), grads)
        key_sum[here, :] += dot_tl(score_grad, query)
        return total + dot(score_grad, keys)

    total = jnp.zeros((rows * group, width), F32)
    total = lax.fori_loop(0, mine, lambda b, c: part(b, False, c), total)
    ends = jnp.where((mine + 1 < chunks) & crosses(starts, first + rows), mine + 2, mine + 1)
    total = lax.fori_loop(mine, ends, lambda b, c: part(b, True, c), total)
    for g in range(group):
        columns = slice(g * width, (g + 1) * width)
        back, gain_part = norm_rope_back(
            raw_q[:, columns],
            gain_q[...],
            cos_here,
            sin_here,
            total[g * rows : (g + 1) * rows] * plain,
        )
        query_grad[:, columns] = back.astype(BF16)
        gain_q_grad[...] += gain_part

    @pl.when(step == chunks - 1)
    def _():
        def drain(c, carry):
            here = pl.ds(pl.multiple_of(place[c] * rows, rows), rows)
            there = pl.ds(pl.multiple_of(c * rows, rows), rows)
            back, gain_part = norm_rope_back(
                raw_k[there, :], gain_k[...], cosine[here, :], sine[here, :],
                key_sum[here, :] * plain,
            )
            key_grad[there, :] = back.astype(BF16)
            value_grad[there, :] = value_sum[here, :].astype(BF16)
            gain_k_grad[...] += gain_part
            return carry

        lax.fori_loop(0, chunks, drain, 0)


def attention_specs(rows, seq_len, group, width):
    by_chunk = pl.BlockSpec((rows, group * width), lambda h, c, *_: (c, h))
    by_head = pl.BlockSpec((seq_len, width), lambda h, c, *_: (0, h))
    table = pl.BlockSpec((seq_len, width), lambda h, c, *_: (0, 0))
    gain = pl.BlockSpec((1, width), lambda h, c, *_: (0, 0))
    return by_chunk, by_head, table, gain


def attend(place, starts, raw_q, raw_k, value, tables, gain_q, gain_k):
    chunks, width = place.shape[0], gain_q.shape[1]
    seq_len = raw_q.shape[0]
    rows, kv_heads = seq_len // chunks, raw_k.shape[1] // width
    group = raw_q.shape[1] // raw_k.shape[1]
    by_chunk, by_head, table, gain = attention_specs(rows, seq_len, group, width)
    return pl.pallas_call(
        functools.partial(attend_kernel, chunks, group, starts.shape[0]),
        grid_spec=pltpu.PrefetchScalarGridSpec(
            num_scalar_prefetch=2,
            grid=(kv_heads, chunks),
            in_specs=[by_chunk, by_head, by_head, table, table, gain, gain],
            out_specs=[by_chunk, by_chunk],
            scratch_shapes=[pltpu.VMEM((seq_len, width), BF16)] * 2,
        ),
        out_shape=[
            jax.ShapeDtypeStruct(raw_q.shape, BF16),
            jax.ShapeDtypeStruct(raw_q.shape, F32),
        ],
        compiler_params=pltpu.CompilerParams(vmem_limit_bytes=48 << 20),
        cost_estimate=pl.CostEstimate(
            flops=2 * seq_len * seq_len * raw_q.shape[1],
            bytes_accessed=14 * raw_q.size,
            transcendentals=seq_len * seq_len,
        ),
        name="attend",
    )(place, starts, raw_q, raw_k, value, *tables, gain_q, gain_k)


def attend_back(place, starts, raw_q, raw_k, value, tables, gain_q, gain_k, attended, log_norm,
                grad):
    chunks, width = place.shape[0], gain_q.shape[1]
    seq_len = raw_q.shape[0]
    rows, kv_heads = seq_len // chunks, raw_k.shape[1] // width
    group = raw_q.shape[1] // raw_k.shape[1]
    by_chunk, by_head, table, gain = attention_specs(rows, seq_len, group, width)
    return pl.pallas_call(
        functools.partial(attend_back_kernel, chunks, group, starts.shape[0]),
        grid_spec=pltpu.PrefetchScalarGridSpec(
            num_scalar_prefetch=2,
            grid=(kv_heads, chunks),
            in_specs=[by_chunk, by_head, by_head, table, table, gain, gain] + [by_chunk] * 3,
            out_specs=[by_chunk, by_head, by_head, gain, gain],
            scratch_shapes=[pltpu.VMEM((seq_len, width), BF16)] * 2
            + [pltpu.VMEM((seq_len, width), F32)] * 2,
        ),
        out_shape=[
            jax.ShapeDtypeStruct(raw_q.shape, BF16),
            jax.ShapeDtypeStruct(raw_k.shape, BF16),
            jax.ShapeDtypeStruct(raw_k.shape, BF16),
            jax.ShapeDtypeStruct((1, width), F32),
            jax.ShapeDtypeStruct((1, width), F32),
        ],
        compiler_params=pltpu.CompilerParams(vmem_limit_bytes=56 << 20),
        cost_estimate=pl.CostEstimate(
            flops=6 * seq_len * seq_len * raw_q.shape[1],
            bytes_accessed=18 * raw_q.size,
            transcendentals=seq_len * seq_len,
        ),
        name="attend_back",
    )(place, starts, raw_q, raw_k, value, *tables, gain_q, gain_k, attended, log_norm, grad)


def rms_back(values, grad):
    inv = inverse_rms(values)
    normed = values * inv
    return (grad - normed * jnp.mean(grad * normed, axis=-1, keepdims=True)) * inv


def gain_sums(wide, narrow):
    size, data = lax.axis_size("mp"), lax.axis_size("dp")
    vector = jnp.concatenate([wide.reshape(-1), narrow.reshape(-1)])
    total = vector
    for k in range(1, size):
        total = total + hop(vector, k)
    count = wide.shape[0]
    spread = total[: wide.size].reshape(count, data, -1)
    small = total[wide.size :]
    me = lax.axis_index("dp")

    def slice_for(device):
        cut = lax.dynamic_index_in_dim(spread, device, 1, keepdims=False)
        return jnp.concatenate([cut.reshape(-1), small])

    result = slice_for(me)
    for k in range(1, data):
        sent = slice_for(lax.rem(me + k, data))
        result = result + lax.ppermute(sent, "dp", [(i, (i + k) % data) for i in range(data)])
    cut_size = wide.size // data
    return result[:cut_size].reshape(count, -1), result[cut_size:].reshape(narrow.shape)


def shards(hidden_in, attn_gain, w_query, key_projection, value_projection, query_gain, key_gain,
           w_out, mlp_gain, w_gate, w_up, w_down, piece_start, out_grad):
    tok_rows = hidden_in.shape[0]
    size = lax.axis_size("mp")
    seq_len = tok_rows * size
    me = lax.axis_index("mp")
    head_dim = query_gain.shape[0]
    q_width, kv_width = w_query.shape[1], key_projection.shape[1]
    place = lax.rem(me - jnp.arange(size, dtype=jnp.int32) + size, size)
    starts = piece_start[0]
    tables = rotary_tables(seq_len, head_dim)
    gain_q = query_gain.astype(F32)[None]
    gain_k = key_gain.astype(F32)[None]

    gains = lax.all_gather(jnp.stack([attn_gain, mlp_gain], axis=0), "dp", axis=1, tiled=True)
    gain_one, gain_two = gains[0].astype(F32), gains[1].astype(F32)
    qkv_all = lax.all_gather(
        jnp.concatenate([w_query, key_projection, value_projection], axis=1),
        "dp", axis=0, tiled=True,
    )

    x_own = hidden_in.astype(F32)
    x_items = ring_gather(hidden_in)
    out_items = [w_out]
    for k in range(size - 1):
        out_items.append(hop(after(out_items[-1], x_items[k]), -1))
    out_all = lax.all_gather(jnp.concatenate(out_items, axis=0), "dp", axis=1, tiled=True)
    gate_all = lax.all_gather(w_gate, "dp", axis=0, tiled=True)
    up_all = lax.all_gather(w_up, "dp", axis=0, tiled=True)
    down_all = lax.all_gather(after(w_down, x_items[2]), "dp", axis=1, tiled=True)

    h_one_items, raw_items = [], []
    for item in x_items:
        rows = item.astype(F32)
        h_one = (rows * inverse_rms(rows) * gain_one).astype(BF16)
        h_one_items.append(h_one)
        raw_items.append(dot(h_one, qkv_all))
    h_one_all = jnp.concatenate(h_one_items, axis=0)
    raw_q = jnp.concatenate([item[:, :q_width] for item in raw_items], axis=0)
    raw_k = jnp.concatenate([item[:, q_width : q_width + kv_width] for item in raw_items], axis=0)
    value = jnp.concatenate(
        [item[:, q_width + kv_width :].astype(BF16) for item in raw_items], axis=0
    )
    cot_items = [out_grad, hop(after(out_grad, x_items[-1]), 1)]
    attended, log_norm = attend(place, starts, raw_q, raw_k, value, tables, gain_q, gain_k)
    attended, cot_items[1] = tied(attended, cot_items[1])

    def chunk(array, k):
        return array[k * tok_rows : (k + 1) * tok_rows]

    own_items = [chunk(attended, 0)] + [hop(chunk(attended, k), -k) for k in range(1, size)]
    attended_own = jnp.concatenate(own_items, axis=1)
    cot_items.append(hop(after(cot_items[1], attended_own), 1))
    x_two = x_own + dot(attended_own, out_all)
    normed_two = x_two * inverse_rms(x_two)
    h_two = (normed_two * gain_two).astype(BF16)
    h_two_items = ring_gather(h_two)
    for _ in range(3, size):
        cot_items.append(hop(after(cot_items[-1], h_two_items[-2]), 1))

    gates, ups, hiddens = [None] * size, [None] * size, [None] * size
    gate_lows, up_lows = [None] * size, [None] * size

    def forward(k):
        gates[k] = dot(h_two_items[k], gate_all)
        ups[k] = dot(h_two_items[k], up_all)
        hiddens[k] = (gates[k] * jax.nn.sigmoid(gates[k]) * ups[k]).astype(BF16)

    def backward(k):
        hidden_grad = dot_tr(cot_items[k], down_all)
        sig = jax.nn.sigmoid(gates[k])
        gate_lows[k] = (
            hidden_grad * ups[k] * (sig * (1.0 + gates[k] * (1.0 - sig)))
        ).astype(BF16)
        up_lows[k] = (hidden_grad * (gates[k] * sig)).astype(BF16)

    for k in range(size):
        forward(k)
        backward(k)

    def h_two_term(k):
        return dot_tr(gate_lows[k], gate_all) + dot_tr(up_lows[k], up_all)

    h_two_all = jnp.concatenate(h_two_items, axis=0)
    cot_all = jnp.concatenate(cot_items, axis=0)
    down_wgrad = dot_tl(jnp.concatenate(hiddens, axis=0), cot_all).astype(BF16)
    gate_wgrad = dot_tl(h_two_all, jnp.concatenate(gate_lows, axis=0)).astype(BF16)
    up_wgrad = dot_tl(h_two_all, jnp.concatenate(up_lows, axis=0)).astype(BF16)
    fillers = {2: down_wgrad, 3: gate_wgrad, 0: up_wgrad}
    h_two_grad = h_two_term(1 % size)
    for k in list(range(2, size)) + [0]:
        arrived = hop(h_two_grad.astype(BF16), 1)
        if k in fillers:
            arrived, fillers[k] = tied(arrived, fillers[k])
        h_two_grad = arrived.astype(F32) + h_two_term(k)
    down_wgrad, gate_wgrad, up_wgrad = fillers[2], fillers[3], fillers[0]

    gain_two_part = jnp.sum(h_two_grad * normed_two, axis=0)
    x_two_grad = out_grad.astype(F32) + rms_back(x_two, h_two_grad * gain_two)
    attn_grad = x_two_grad.astype(BF16)
    attended_grad_own = dot_tr(attn_grad, out_all).astype(BF16)
    grad_items = [attended_grad_own[:, :q_width]] + [
        hop(attended_grad_own[:, k * q_width : (k + 1) * q_width], k) for k in range(1, size)
    ]
    attended_grad = jnp.concatenate(grad_items, axis=0)
    out_wgrad = dot_tl(attended_own, attn_grad).astype(BF16)
    attended_grad, out_wgrad = tied(attended_grad, out_wgrad)

    def mlp_term(k):
        return dot(hiddens[k], down_all)

    mlp_sum = mlp_term(1 % size)
    for count, k in enumerate(list(range(2, size)) + [0]):
        mlp_sum = after(mlp_sum.astype(BF16), attended_grad if count else h_two_grad)
        mlp_sum = hop(mlp_sum, 1)
        mlp_sum = mlp_sum.astype(F32) + mlp_term(k)
    block_out = (x_two + mlp_sum.astype(BF16).astype(F32)).astype(BF16)

    query_grad, key_grad, value_grad, gain_q_part, gain_k_part = attend_back(
        place, starts, raw_q, raw_k, value, tables, gain_q, gain_k, attended, log_norm,
        attended_grad,
    )
    qkv_grad = jnp.concatenate([query_grad, key_grad, value_grad], axis=1)
    h_one_grad = dot_tr(chunk(qkv_grad, 1 % size), qkv_all)
    qkv_wgrad = dot_tl(h_one_all, qkv_grad).astype(BF16)
    first = True
    for k in list(range(2, size)) + [0]:
        arrived = hop(h_one_grad.astype(BF16), 1)
        if first:
            arrived, qkv_wgrad = tied(arrived, qkv_wgrad)
        first = False
        h_one_grad = arrived.astype(F32) + dot_tr(chunk(qkv_grad, k), qkv_all)

    normed_one = x_own * inverse_rms(x_own)
    gain_one_part = jnp.sum(h_one_grad * normed_one, axis=0)
    in_grad = x_two_grad + rms_back(x_own, h_one_grad * gain_one)

    def scatter(array, dim):
        return lax.psum_scatter(array, "dp", scatter_dimension=dim, tiled=True)

    down_sum = scatter(down_wgrad, 1).astype(F32)
    gate_sum = scatter(gate_wgrad, 0).astype(F32)
    up_sum = scatter(up_wgrad, 0).astype(F32)
    out_cut = scatter(out_wgrad, 1)
    block = w_out.shape[0]
    out_sum = out_cut[:block].astype(F32)
    for k in range(1, size):
        out_sum = out_sum + hop(out_cut[k * block : (k + 1) * block], k).astype(F32)
    qkv_sum = scatter(qkv_wgrad, 0).astype(F32)

    wide, narrow = gain_sums(
        jnp.stack([gain_one_part, gain_two_part]),
        jnp.concatenate([gain_q_part, gain_k_part], axis=0),
    )
    return (
        block_out, in_grad, wide[0],
        qkv_sum[:, :q_width], qkv_sum[:, q_width : q_width + kv_width],
        qkv_sum[:, q_width + kv_width :],
        narrow[0], narrow[1], out_sum, wide[1], gate_sum, up_sum, down_sum,
    )


def solution(mesh):
    both = P(("dp", "mp"), None)
    weight, turned = P("dp", "mp"), P("mp", "dp")
    return jax.shard_map(
        shards,
        mesh=mesh,
        in_specs=(
            both, P("dp"), weight, weight, weight, P(), P(), turned, P("dp"), weight, weight,
            turned, P("dp", None), both,
        ),
        out_specs=(
            both, both, P("dp"), weight, weight, weight, P(), P(), turned, P("dp"), weight, weight,
            turned,
        ),
        check_vma=False,
    )
```
